32 devices in a mesh: aa: 16 (over z, y, core), ba: 2 (over x).
Axes of the slice: x: 2, y: 2, z: 4, core: 2. Of those that a mesh axis runs over, the one named last changes fastest.
Arguments:
- inputs: bfloat16 [8192, 3584], P('aa', 'ba'), may hold values from -6 to 6
- cotangent: bfloat16 [8192, 3584], P('aa', 'ba'), may hold values from -6 to 6
- base_weight: bfloat16 [3584, 3584], P(None, 'ba'), may hold values from -0.09375 to 0.09375
- adapter_ids: int32 [8192, 1], P('aa'), may hold values from 0 to 63; in each aligned block of 512 rows (0 to 511, 512 to 1023, ...) at most 16 rows name the same one
- adapters: float32 [64, 2, 16, 3584], P('aa', None, None, 'ba'), may hold values from -0.09375 to 0.09375
- first_moment: float32 [64, 2, 16, 3584], P('aa', None, None, 'ba'), may hold values from -3 to 3
- second_moment: float32 [64, 2, 16, 3584], P('aa', None, None, 'ba'), may hold values from 0.05 to 1
Outputs:
- input_gradient: bfloat16 [8192, 3584], P('aa', 'ba')
- new_adapters: float32 [64, 2, 16, 3584], P('aa', None, None, 'ba')
- new_first: float32 [64, 2, 16, 3584], P('aa', None, None, 'ba')
- new_second: float32 [64, 2, 16, 3584], P('aa', None, None, 'ba')
- grad_norm: float32 [], replicated
The draws below stay inside these ranges and needn't reach their ends.
Inputs may be any that keep to these rules, and one draw needn't show every extreme that they name: `adapter_ids`: in the rows of one device no adapter is named by more than 16 tokens, a bound that some block reaches; every adapter is named somewhere.
All inputs are finite; a program needn't handle non-finite values.
Results may differ from the reference program's by a relative error of at most 0.0034.
Values may be sent and summed in bfloat16 or wider, within the bound.
No kernel may reach another device: no remote copies, remote signals or barrier semaphores. Data moves between devices by JAX's collectives and lax.ppermute only.
A program may use at most 128 MiB of HBM per device.

```python
import math
import jax
import jax.numpy as jnp
import numpy as np
from jax import lax

MODEL_WIDTH = 3584
R = 16
TOK_DEV = 512
ADAPTERS = 64
MOST = 16
TOKENS = 8192
N_AA = 16


def block_scale(stream_key, dims, cuts, smallest, largest):
    factor_of = 1.0
    for dim, blocks in cuts:
        steps = jax.random.uniform(jax.random.fold_in(jax.random.fold_in(stream_key, 6), dim), (blocks,), jnp.float32, smallest / len(cuts), largest / len(cuts))
        factor_of = factor_of * jnp.repeat(jnp.exp(steps), dims[dim] // blocks).reshape((-1,) + (1,) * (len(dims) - 1 - dim))
    return factor_of


def routed_block(stream_key, own, number, rows, count, top, limit, slope):
    sequence = jax.random.permutation(stream_key, count)
    crowded, ordinary = portions_of(count, rows * top, limit, slope, True), portions_of(count, rows * top, limit, slope, False)
    places = jnp.arange(count)

    def named(sizes, rotation):
        used = int((sizes > 0).sum())
        fixed = max(1, used // 4)
        moved = fixed + (places - fixed + rotation * (used - fixed)) % max(1, count - fixed)
        return jnp.zeros((count,), jnp.int32).at[sequence[jnp.where(places < fixed, places, moved)]].set(jnp.asarray(sizes, jnp.int32))

    sizes = jnp.where(number % 4 == 0, named(crowded, number // 4), named(ordinary, number - number // 4 - 1))
    mixed = jax.random.permutation(jax.random.fold_in(own, 3), count)
    giver, taker = mixed[0:count // 2 * 2:2], mixed[1:count // 2 * 2:2]
    room = jnp.minimum(sizes[giver] - 1, limit - sizes[taker]) // 2
    room = jnp.where((giver == sequence[0]) | (taker == sequence[0]) | (sizes[taker] == 0), 0, jnp.maximum(room, 0))
    moved = jax.random.randint(jax.random.fold_in(own, 4), (count // 2,), 0, 1 << 20) % (room + 1)
    sizes = sizes.at[giver].add(-moved).at[taker].add(moved)
    members = jnp.searchsorted(jnp.cumsum(sizes), jnp.arange(rows * top), side="right").astype(jnp.int32)
    table = members.reshape(top, rows).T
    table = table[jax.random.permutation(jax.random.fold_in(own, 1), rows)]
    rotation = jax.random.randint(jax.random.fold_in(own, 2), (rows, 1), 0, top)
    return jnp.take_along_axis(table, (jnp.arange(top)[None, :] + rotation) % top, axis=1)


def portions_of(number_of, total, reach, lean, full):
    portions = [(1 << 20) // math.isqrt(standing ** lean) + 1 for standing in range(1, number_of + 1)]
    largest = reach if full else min(reach, max(-(-total // number_of), total * portions[0] // sum(portions)))
    least = 1 if total - largest >= number_of - 1 else 0
    given, spare = [largest] + [least] * (number_of - 1), total - largest - least * (number_of - 1)
    while spare > 0:
        candidates = [i for i in range(1, number_of) if given[i] < largest] or [i for i in range(1, number_of) if given[i] < reach]
        pool, left = sum([portions[i] for i in candidates]), spare
        for i in candidates:
            addition = min(reach - given[i], max(1, left * portions[i] // pool), spare)
            given[i] = given[i] + addition
            spare = spare - addition
    return np.array(given)


def bell_draw(stream_key, extent, spread, reach, split=(), held_as=jnp.bfloat16):
    values = spread * jax.random.normal(stream_key, extent, jnp.float32)
    if split:
        values = values * block_scale(stream_key, extent, split, -0.22, 0.18)
    return jnp.clip(values, -reach, reach).astype(held_as)


def setup_inputs(seed: int = 0) -> dict:
    seeds = jax.random.split(jax.random.key(seed), 8)
    inputs = bell_draw(seeds[0], (TOKENS, MODEL_WIDTH), 1.0, 6.0, ((0, 16), (1, 2)))
    cotangent = bell_draw(seeds[1], (TOKENS, MODEL_WIDTH), 1.0, 6.0, ((0, 16), (1, 2)))
    base_weight = bell_draw(seeds[2], (MODEL_WIDTH, MODEL_WIDTH), MODEL_WIDTH ** -0.5, 0.09375, ((1, 2),))
    adapter_ids_keys = jax.random.split(jax.random.fold_in(seeds[3], 1), TOKENS // TOK_DEV)
    adapter_ids_turns = jax.random.permutation(jax.random.fold_in(seeds[3], 3), TOKENS // TOK_DEV)
    adapter_ids = jax.vmap(lambda own, number: routed_block(jax.random.fold_in(seeds[3], 2), own, number, TOK_DEV, ADAPTERS, 1, MOST, 2))(adapter_ids_keys, adapter_ids_turns).reshape((TOKENS, 1))
    adapters = bell_draw(seeds[4], (ADAPTERS, 2, R, MODEL_WIDTH), MODEL_WIDTH ** -0.5, 0.09375, ((0, 16), (3, 2)), jnp.float32)
    first_moment = bell_draw(seeds[5], (ADAPTERS, 2, R, MODEL_WIDTH), 0.2, 3.0, ((0, 16), (3, 2)), jnp.float32)
    second_moment = jnp.clip(jnp.exp(math.log(1.0) - 2.9957323 * jax.random.uniform(seeds[6], (ADAPTERS, 2, R, MODEL_WIDTH), jnp.float32) ** block_scale(seeds[6], (ADAPTERS, 2, R, MODEL_WIDTH), ((0, 16), (3, 2)), -0.2, 0.2)), 0.05, 1.0)
    return dict(inputs=inputs, cotangent=cotangent, base_weight=base_weight, adapter_ids=adapter_ids, adapters=adapters, first_moment=first_moment, second_moment=second_moment)


adapter_scale = 2.0
beta_first = 0.9
beta_second = 0.999
adam_eps = 1e-08
learn_rate = 0.01
bias_first = 1.0 - math.exp(1000.0 * math.log(beta_first))
bias_second = 1.0 - math.exp(1000.0 * math.log(beta_second))

def adam_update(adapters, first_moment, second_moment, gradients, squares):
    clip_limit = math.sqrt(2.0 * R * MODEL_WIDTH)
    clip_factor = clip_limit / jnp.maximum(jnp.sqrt(squares), clip_limit)
    clipped = gradients * clip_factor[:, None, None, None]
    new_first = beta_first * first_moment + (1.0 - beta_first) * clipped
    new_second = beta_second * second_moment + (1.0 - beta_second) * clipped * clipped
    update = new_first / bias_first / (jnp.sqrt(new_second / bias_second) + adam_eps)
    return (adapters - learn_rate * update, new_first, new_second)

def adapter_grouped(pieces):
    incoming_rows, cotangent_rows, down_full, up_full = pieces
    down_reduced = down_full.astype(jnp.bfloat16)
    up_low = up_full.astype(jnp.bfloat16)
    projected = jnp.dot(incoming_rows, down_reduced.T, preferred_element_type=jnp.float32)
    pulled = jnp.dot(cotangent_rows, up_low.T, preferred_element_type=jnp.float32)
    projection_reduced = projected.astype(jnp.bfloat16)
    fetched_reduced = pulled.astype(jnp.bfloat16)
    down_gradient = adapter_scale * jnp.dot(fetched_reduced.T, incoming_rows, preferred_element_type=jnp.float32)
    up_gradient = adapter_scale * jnp.dot(projection_reduced.T, cotangent_rows, preferred_element_type=jnp.float32)
    adapter_rows = (adapter_scale * jnp.dot(fetched_reduced, down_reduced, preferred_element_type=jnp.float32)).astype(jnp.bfloat16)
    return (down_gradient, up_gradient, adapter_rows)

def reference(inputs, cotangent, base_weight, adapter_ids, adapters, first_moment, second_moment):
    chosen = adapter_ids[:, 0].astype(jnp.int32)
    blocks = chosen.reshape(N_AA, TOK_DEV)
    counter = jnp.arange(TOK_DEV, dtype=jnp.int32)
    matches = (blocks[:, :, None] == blocks[:, None, :]) & (counter[None, None, :] < counter[None, :, None])
    slot_rank = lax.optimization_barrier(jnp.sum(matches.astype(jnp.int32), axis=2))
    block_index = jnp.arange(N_AA, dtype=jnp.int32)[:, None]
    token_position = (blocks * (N_AA * MOST) + block_index * MOST + slot_rank).reshape(-1).astype(jnp.int32)
    slot_overall = ADAPTERS * N_AA * MOST
    incoming_rows = jnp.zeros((slot_overall, MODEL_WIDTH), jnp.bfloat16).at[token_position].set(inputs).reshape(ADAPTERS, N_AA * MOST, MODEL_WIDTH)
    cotangent_rows = jnp.zeros((slot_overall, MODEL_WIDTH), jnp.bfloat16).at[token_position].set(cotangent).reshape(ADAPTERS, N_AA * MOST, MODEL_WIDTH)
    down_gradient, up_gradient, adapter_rows = lax.map(adapter_grouped, (incoming_rows, cotangent_rows, adapters[:, 0], adapters[:, 1]))
    adapter_local = adapter_rows.reshape(slot_overall, MODEL_WIDTH)[token_position]
    frozen_term = jnp.dot(cotangent, base_weight.T, preferred_element_type=jnp.float32)
    input_gradient = (frozen_term + adapter_local.astype(jnp.float32)).astype(jnp.bfloat16)
    gradients = jnp.stack([down_gradient, up_gradient], axis=1)
    squares = lax.optimization_barrier(jnp.sum(gradients * gradients, axis=(1, 2, 3)))
    new_adapters, new_first, new_second = adam_update(adapters, first_moment, second_moment, gradients, squares)
    return (input_gradient, new_adapters, new_first, new_second, jnp.sqrt(jnp.sum(squares)))
```

```python
import math

import jax
import jax.numpy as jnp
from jax import lax
from jax.sharding import PartitionSpec as P

adapter_scale = 2.0
beta_first = 0.9
beta_second = 0.999
adam_eps = 1e-08
learn_rate = 0.01
bias_first = 1.0 - math.exp(1000.0 * math.log(beta_first))
bias_second = 1.0 - math.exp(1000.0 * math.log(beta_second))

bf16 = jnp.bfloat16
f32 = jnp.float32


def dot(a, b, ca, cb):
    return lax.dot_general(a, b, (((ca,), (cb,)), ((), ())), preferred_element_type=f32)


def make_local(n_aa, n_ba):
    nc = 2 if n_aa % 2 == 0 else 1
    ny = 2 if (n_aa // nc) % 2 == 0 else 1
    nz = n_aa // (nc * ny)

    def place(z, y, c):
        return (z * ny + y) * nc + c

    cells = [(z, y, c) for z in range(nz) for y in range(ny) for c in range(nc)]
    core_pairs = [(place(z, y, c), place(z, y, nc - 1 - c)) for z, y, c in cells]
    row_pairs = [(place(z, y, c), place(z, ny - 1 - y, c)) for z, y, c in cells]
    ring_pairs = [(place((z + 1) % nz, y, c), place(z, y, c)) for z, y, c in cells]

    def core_swap(a):
        return lax.ppermute(a, "aa", core_pairs)

    def row_swap(a):
        return lax.ppermute(a, "aa", row_pairs)

    def ring(a):
        return lax.ppermute(a, "aa", ring_pairs)

    def shift_ba(a, k):
        return lax.ppermute(a, "ba", [(i, (i + k) % n_ba) for i in range(n_ba)])

    def local(inputs, cotangent, base_weight, adapter_ids, adapters, first_moment, second_moment):
        tokens, width = inputs.shape
        count, _, rank, _ = adapters.shape
        rows = count * rank
        me = lax.axis_index("aa")
        my_core = me % nc
        my_row = (me // nc) % ny
        my_z = me // (nc * ny)
        my_ba = lax.axis_index("ba")

        low = adapters.astype(bf16)
        down = low[:, 0].reshape(rows, width)
        up = low[:, 1].reshape(rows, width)

        z_up, z_down, y_up, y_down = [up], [down], [], []
        for k in range(nz):
            y_up.append(row_swap(z_up[k]))
            y_down.append(row_swap(z_down[k]))
            if k < nz - 1:
                z_up.append(ring(z_up[k]))
                z_down.append(ring(z_down[k]))
        up_all = jnp.concatenate([v for k in range(nz) for v in (z_up[k], y_up[k])][: nz * ny], 0)
        down_all = jnp.concatenate([v for k in range(nz) for v in (z_down[k], y_down[k])][: nz * ny], 0)
        groups = nz * ny

        x_par, c_par, id_par = core_swap(inputs), core_swap(cotangent), core_swap(adapter_ids)

        def frozen(target):
            piece = lax.dynamic_slice_in_dim(base_weight, target * width, width, 0)
            return dot(cotangent, piece, 1, 1)

        received = []
        for k in range(1, n_ba):
            received.append(shift_ba(frozen((my_ba + k) % n_ba).astype(bf16), k))
        own_frozen = frozen(my_ba)

        names = []
        for k in range(nz):
            for other in range(ny):
                y = my_row if other == 0 else ny - 1 - my_row
                owner = (((my_z + k) % nz) * ny + y) * nc + my_core
                names.append(owner * count + jnp.arange(count, dtype=jnp.int32))
        names = jnp.concatenate(names)
        ids_own, ids_par = adapter_ids[:, 0], id_par[:, 0]
        mask_own = names[:, None] == ids_own[None, :]
        mask_par = names[:, None] == ids_par[None, :]

        def project(table, toks, mask):
            full = dot(table, toks, 1, 1).reshape(groups * count, rank, tokens)
            return jnp.sum(jnp.where(mask[:, None, :], full, 0.0), axis=0)

        partial = jnp.stack(
            [
                project(up_all, cotangent, mask_own),
                project(up_all, c_par, mask_par),
                project(down_all, inputs, mask_own),
                project(down_all, x_par, mask_par),
            ]
        )
        total = partial
        for k in range(1, n_ba):
            total = total + shift_ba(partial, k)
        lows = (adapter_scale * total.astype(bf16)).astype(bf16)

        def spread(values, mask):
            return jnp.where(mask[:, None, :], values[None], jnp.zeros((), bf16)).reshape(
                groups * rows, tokens
            )

        pull_own, pull_par = spread(lows[0], mask_own), spread(lows[1], mask_par)
        proj_own, proj_par = spread(lows[2], mask_own), spread(lows[3], mask_par)

        def gradient(k, own_left, par_left, own_right, par_right):
            lo, hi = k * ny * rows, (k + 1) * ny * rows
            return dot(own_left[lo:hi], own_right, 1, 0) + dot(par_left[lo:hi], par_right, 1, 0)

        def reduced(own_left, par_left, own_right, par_right):
            def row_sum(k):
                g = gradient(k, own_left, par_left, own_right, par_right)
                if ny == 1:
                    return g
                return g[:rows] + row_swap(g[rows:].astype(bf16)).astype(f32)

            acc = row_sum(1 % nz)
            for s in range(1, nz):
                acc = ring(acc.astype(bf16)).astype(f32) + row_sum((s + 1) % nz)
            return acc

        grad_down = reduced(pull_own, pull_par, inputs, x_par)
        grad_up = reduced(proj_own, proj_par, cotangent, c_par)

        lora_own = dot(pull_own, down_all, 0, 0).astype(bf16)
        lora_par = core_swap(dot(pull_par, down_all, 0, 0).astype(bf16))
        result = own_frozen
        for piece in received:
            result = result + piece.astype(f32)
        input_gradient = (result + (lora_own.astype(f32) + lora_par.astype(f32))).astype(bf16)

        gradients = jnp.stack(
            [grad_down.reshape(count, rank, width), grad_up.reshape(count, rank, width)], axis=1
        )
        part = jnp.sum(gradients * gradients, axis=(1, 2, 3))
        squares = part
        for k in range(1, n_ba):
            squares = squares + shift_ba(part, k)
        grand_total = lax.psum(jnp.sum(part), ("aa", "ba"))

        clip_limit = math.sqrt(2.0 * rank * width * n_ba)
        clip_factor = clip_limit / jnp.maximum(jnp.sqrt(squares), clip_limit)
        clipped = gradients * clip_factor[:, None, None, None]
        new_first = beta_first * first_moment + (1.0 - beta_first) * clipped
        new_second = beta_second * second_moment + (1.0 - beta_second) * clipped * clipped
        update = new_first / bias_first / (jnp.sqrt(new_second / bias_second) + adam_eps)
        new_adapters = adapters - learn_rate * update
        return (input_gradient, new_adapters, new_first, new_second, jnp.sqrt(grand_total))

    return local


def solution(mesh):
    local = make_local(mesh.shape["aa"], mesh.shape["ba"])
    moments = P("aa", None, None, "ba")
    in_specs = (P("aa", "ba"), P("aa", "ba"), P(None, "ba"), P("aa", None), moments, moments, moments)
    out_specs = (P("aa", "ba"), moments, moments, moments, P())
    return jax.shard_map(local, mesh=mesh, in_specs=in_specs, out_specs=out_specs, check_vma=False)
```
